128 devices in a mesh: branch: 2 (over core), seq: 32 (over z, y, x_lo), mp: 2 (over x_hi).
Axes of the slice: x: 4 (x_hi: 2, x_lo: 2; x = x_hi * 2 + x_lo), y: 4, z: 4, core: 2. Of those that a mesh axis runs over, the one named last changes fastest.
Arguments:
- tokens: bfloat16 [8192, 4096], P('seq', 'mp'), may hold values from -6 to 6
- light_in: bfloat16 [4096, 2048], P(None, ('branch', 'mp')), may hold values from -0.09375 to 0.09375
- light_out: bfloat16 [2048, 4096], P(('branch', 'mp')), may hold values from -0.1875 to 0.1875
- heavy_in: bfloat16 [4096, 16384], P(None, ('branch', 'seq', 'mp')), may hold values from -0.09375 to 0.09375
- heavy_out: bfloat16 [16384, 4096], P(('branch', 'seq', 'mp')), may hold values from -0.1875 to 0.1875
- route_index: int32 [32, 32], P('seq'), may hold values from 0 to 255, as said below
- route_count: int32 [32], P('seq'), may hold values from 1 to 32, as said below
- route_gate: float32 [32, 32], P('seq'), may hold values from 0.25 to 2
- cotangent: bfloat16 [8192, 4096], P('seq', 'mp'), may hold values from -6 to 6
Outputs:
- mixed: bfloat16 [8192, 4096], P('seq', ('branch', 'mp'))
- grad_heavy_in: bfloat16 [4096, 16384], P(None, ('branch', 'seq', 'mp'))
- grad_heavy_out: bfloat16 [16384, 4096], P(('branch', 'seq', 'mp'))
The draws below stay inside these ranges and needn't reach their ends.
Inputs may be any that keep to these rules, and one draw needn't show every extreme that they name: `route_index`: each row holds 32 distinct positions of its shard. The first route_count[s] slots of shard s are live; some shard has all 32 slots live.
All inputs are finite; a program needn't handle non-finite values.
Results may differ from the reference program's by a relative error of at most 0.008.
Values may be sent and summed in bfloat16 or wider, within the bound.
No kernel may reach another device: no remote copies, remote signals or barrier semaphores. Data moves between devices by JAX's collectives and lax.ppermute only.
A program may use at most 128 MiB of HBM per device.

```python
import math
import jax
import jax.numpy as jnp

D = 4096
FFL = 2048
FFH = 16384
TOK_DEV = 256
CAP = 32
TOKENS = 8192
N_SEQ = 32


def draw_route_index(key, part):
    shards = TOKENS // TOK_DEV
    keys = jax.random.split(jax.random.fold_in(key, 11), shards)

    def one_shard(shard_key):
        return jax.random.permutation(shard_key, TOK_DEV)[:CAP]
    return jax.vmap(one_shard)(keys).astype(jnp.int32)


def draw_route_count(key, part):
    shards = TOKENS // TOK_DEV
    lowest = max(CAP // 3, 1)
    counts = jax.random.randint(jax.random.fold_in(key, 21), (shards,), lowest, CAP + 1)
    filled = jax.random.randint(jax.random.fold_in(key, 22), (), 0, shards)
    counts = jnp.where(jnp.arange(shards) == filled, CAP, counts)
    return counts.astype(jnp.int32)


def strengthened(array, rng, source, target, parts, factor):
    def block_of(axis_at):
        return (jnp.arange(array.shape[axis_at]) // (array.shape[axis_at] // parts)).reshape((-1,) + (1,) * (array.ndim - 1 - axis_at))

    first = jax.random.permutation(rng, parts)[block_of(target)]
    second = (block_of(target) + parts // 2) % parts
    return jnp.where((block_of(source) == first) | (block_of(source) == second), factor * array, array)


def levels(rng, dims, pieces, smallest, largest):
    level = 1.0
    for axis_at, blocks in pieces:
        draws = jax.random.uniform(jax.random.fold_in(jax.random.fold_in(rng, 6), axis_at), (blocks,), jnp.float32, smallest / len(pieces), largest / len(pieces))
        level = level * jnp.repeat(jnp.exp(draws), dims[axis_at] // blocks).reshape((-1,) + (1,) * (len(dims) - 1 - axis_at))
    return level


def gaussian(own_key, dims, width, most, cuts=(), kind=jnp.bfloat16):
    result = width * jax.random.normal(own_key, dims, jnp.float32)
    if cuts:
        result = result * levels(own_key, dims, cuts, -0.22, 0.18)
    return jnp.clip(result, -most, most).astype(kind)


def gaussian_with(key, shape, spread, bound, cuts, heavy, kind=jnp.bfloat16):
    values = spread * jax.random.normal(key, shape, jnp.float32)
    if cuts:
        values = values * levels(key, shape, cuts, -0.22, 0.18)
    return jnp.clip(strengthened(values, jax.random.fold_in(key, 3), *heavy), -bound, bound).astype(kind)


def setup_inputs(seed: int = 0) -> dict:
    seeds = jax.random.split(jax.random.key(seed), 10)
    tokens = gaussian(seeds[0], (TOKENS, D), 1.0, 6.0, ((0, 32), (1, 2)))
    light_in = gaussian(seeds[1], (D, FFL), D ** -0.5, 0.09375, ((1, 4),))
    light_out = gaussian_with(seeds[2], (FFL, D), FFL ** -0.5, 0.1875, ((0, 4),), (0, 1, 4, 2.0))
    heavy_in = gaussian(seeds[3], (D, FFH), D ** -0.5, 0.09375, ((1, 128),))
    heavy_out = gaussian_with(seeds[4], (FFH, D), FFH ** -0.5, 0.1875, ((0, 128),), (0, 1, 128, 5.5))
    route_index = draw_route_index(jax.random.fold_in(seeds[9], 71), 0)
    route_count = draw_route_count(jax.random.fold_in(seeds[9], 71), 0)
    route_gate = jnp.clip(jnp.exp(math.log(2.0) - 2.0794415 * jax.random.uniform(seeds[7], (N_SEQ, CAP), jnp.float32) ** levels(seeds[7], (N_SEQ, CAP), ((0, 32),), -0.2, 0.2)), 0.25, 2.0)
    cotangent = gaussian(seeds[8], (TOKENS, D), 1.0, 6.0, ((0, 32), (1, 2)))
    return dict(tokens=tokens, light_in=light_in, light_out=light_out, heavy_in=heavy_in, heavy_out=heavy_out, route_index=route_index, route_count=route_count, route_gate=route_gate, cotangent=cotangent)


root_coef = 0.7978845608
cubic_coef = 0.044715


def gelu_tanh(values):
    inner = root_coef * (values + cubic_coef * values * values * values)
    return 0.5 * values * (1.0 + jnp.tanh(inner))


def gelu_slope(values):
    tangent = jnp.tanh(root_coef * (values + cubic_coef * values * values * values))
    return 0.5 * (1.0 + tangent) + 0.5 * values * (1.0 - tangent * tangent) * root_coef * (1.0 + 3.0 * cubic_coef * values * values)


def reference(tokens, light_in, light_out, heavy_in, heavy_out, route_index, route_count, route_gate, cotangent):
    light_hidden = gelu_tanh(jnp.dot(tokens, light_in, preferred_element_type=jnp.float32)).astype(jnp.bfloat16)
    light_y = jnp.dot(light_hidden, light_out, preferred_element_type=jnp.float32)
    shard_base = (jnp.arange(N_SEQ, dtype=jnp.int32) * TOK_DEV)[:, None]
    picked_rows = (route_index.astype(jnp.int32) + shard_base).reshape(-1)
    live_slots = jnp.arange(CAP, dtype=jnp.int32)[None, :] < route_count[:, None]
    row_scale = jnp.where(live_slots, route_gate, jnp.zeros_like(route_gate)).reshape(-1)
    picked = tokens[picked_rows]
    pre_act = jnp.dot(picked, heavy_in, preferred_element_type=jnp.float32)
    heavy_hidden = gelu_tanh(pre_act).astype(jnp.bfloat16)
    heavy_y = jnp.dot(heavy_hidden, heavy_out, preferred_element_type=jnp.float32) * row_scale[:, None]
    mixed = light_y.at[picked_rows].add(heavy_y).astype(jnp.bfloat16)
    back_rows = (cotangent[picked_rows].astype(jnp.float32) * row_scale[:, None]).astype(jnp.bfloat16)
    grad_heavy_out = jnp.dot(heavy_hidden.T, back_rows, preferred_element_type=jnp.float32).astype(jnp.bfloat16)
    slope = (jnp.dot(back_rows, heavy_out.T, preferred_element_type=jnp.float32) * gelu_slope(pre_act)).astype(jnp.bfloat16)
    grad_heavy_in = jnp.dot(picked.T, slope, preferred_element_type=jnp.float32).astype(jnp.bfloat16)
    return mixed, grad_heavy_in, grad_heavy_out
```

```python
import jax
import jax.numpy as jnp
from jax import lax
from jax.sharding import Mesh, PartitionSpec as P

root_coef = 0.7978845608
cubic_coef = 0.044715

swap = [(0, 1), (1, 0)]


def gelu_tanh(values):
    inner = root_coef * (values + cubic_coef * values * values * values)
    return 0.5 * values * (1.0 + jnp.tanh(inner))


def gelu_slope(values):
    tangent = jnp.tanh(root_coef * (values + cubic_coef * values * values * values))
    return 0.5 * (1.0 + tangent) + 0.5 * values * (1.0 - tangent * tangent) * root_coef * (
        1.0 + 3.0 * cubic_coef * values * values
    )


def dot(left, right):
    return jnp.dot(left, right, preferred_element_type=jnp.float32)


def general(left, right, left_dims, right_dims):
    return lax.dot_general(
        left, right, ((left_dims, right_dims), ((), ())), preferred_element_type=jnp.float32
    )


def part(x, index, size, dim):
    return lax.dynamic_slice_in_dim(x, index * size, size, axis=dim)


def ordered(first, mine, other, dim):
    return jnp.where(
        first, jnp.concatenate([mine, other], dim), jnp.concatenate([other, mine], dim)
    )


def per_device(
    tokens,
    light_in,
    light_out,
    heavy_in,
    heavy_out,
    route_index,
    route_count,
    route_gate,
    cotangent,
):
    core = lax.axis_index("b")
    side = lax.axis_index("xh")
    rows, width = tokens.shape
    slots = route_index.shape[1]
    half = slots // 2

    positions = route_index[0]
    live_slots = jnp.arange(slots, dtype=jnp.int32) < route_count[0]
    row_scale = jnp.where(live_slots, route_gate[0], jnp.zeros_like(route_gate[0]))
    own_positions = part(positions, core, half, 0)
    own_scale = part(row_scale, core, half, 0)
    picked = jnp.take(tokens, own_positions, axis=0, mode="clip")
    back = jnp.take(cotangent, own_positions, axis=0, mode="clip").astype(jnp.float32)
    back = (back * own_scale[:, None]).astype(jnp.bfloat16)
    routed = jnp.concatenate([picked, back], axis=1)
    routed = lax.all_gather(routed, ("xh", "xl", "y", "z", "b"), axis=0, tiled=True)
    routed = routed.reshape(2, routed.shape[0] // 2, 2 * width)

    block = heavy_out.shape[1] // 4
    pieces = []
    for core_off in (0, 1):
        for side_off in (0, 1):
            target = (core ^ core_off) * 2 + (side ^ side_off)
            piece = part(heavy_out, target, block, 1)
            if core_off or side_off:
                pairs = [(k, k ^ (core_off * 2 + side_off)) for k in range(4)]
                piece = lax.ppermute(piece, ("b", "xh"), pairs)
            pieces.append(piece)
    group_weight = jnp.concatenate(pieces, axis=0)

    sent = part(tokens, core, rows // 2, 0)
    got = lax.ppermute(sent, "xh", swap)
    other = ordered(core == 0, got, lax.ppermute(got, "b", swap), 0)
    whole = ordered(side == 0, tokens, other, 1)
    light_hidden = gelu_tanh(dot(whole, light_in)).astype(jnp.bfloat16)
    mine = dot(light_hidden, part(light_out, core, width, 1))
    theirs = dot(light_hidden, part(light_out, 1 - core, width, 1))
    chip_terms = mine + lax.ppermute(theirs, "b", swap)
    light_share = part(chip_terms, side, block, 1) + lax.ppermute(
        part(chip_terms, 1 - side, block, 1).astype(jnp.bfloat16), "xh", swap
    ).astype(jnp.float32)

    in_weight = heavy_in.reshape(2, width, heavy_in.shape[1])
    out_weight = heavy_out
    pre_act = dot(routed[0, :, :width], in_weight[0]) + dot(routed[1, :, :width], in_weight[1])
    heavy_hidden = gelu_tanh(pre_act).astype(jnp.bfloat16)
    across = lax.ppermute(heavy_hidden, "xh", swap)
    pair = jnp.concatenate([heavy_hidden, across], axis=1)
    group_hidden = jnp.concatenate([pair, lax.ppermute(pair, "b", swap)], axis=1)
    partial_terms = dot(group_hidden, group_weight).astype(jnp.bfloat16)
    arrived = lax.all_to_all(partial_terms, ("xl", "y", "z"), 0, 0, tiled=True)
    homed = arrived.reshape(-1, slots, block).astype(jnp.float32).sum(axis=0)
    heavy_share = homed * row_scale[:, None]
    mixed = light_share.at[positions].add(heavy_share).astype(jnp.bfloat16)

    grad_out = jnp.concatenate(
        [general(heavy_hidden, routed[k, :, width:], (0,), (0,)) for k in (0, 1)], axis=1
    ).astype(jnp.bfloat16)
    slope = general(routed[0, :, width:], out_weight[:, :width], (1,), (1,)) + general(
        routed[1, :, width:], out_weight[:, width:], (1,), (1,)
    )
    slope = (slope * gelu_slope(pre_act)).astype(jnp.bfloat16)
    grad_in = jnp.concatenate(
        [general(routed[k, :, :width], slope, (0,), (0,)) for k in (0, 1)], axis=0
    ).astype(jnp.bfloat16)
    return (mixed, grad_in, grad_out)


def solution(mesh):
    split = Mesh(mesh.devices.reshape(2, 4, 4, 2, 2), ("b", "z", "y", "xl", "xh"))
    seq = ("z", "y", "xl")
    units = ("b", "z", "y", "xl", "xh")
    in_specs = (
        P(seq, "xh"),
        P(None, ("b", "xh")),
        P(("b", "xh"), None),
        P(None, units),
        P(units, None),
        P(seq, None),
        P(seq),
        P(seq, None),
        P(seq, "xh"),
    )
    out_specs = (
        P(seq, ("b", "xh")),
        P(None, units),
        P(units, None),
    )
    return jax.shard_map(
        per_device, mesh=split, in_specs=in_specs, out_specs=out_specs, check_vma=False
    )
```

```python
import itertools

import jax
import jax.numpy as jnp
from jax import lax
from jax.sharding import Mesh, PartitionSpec as P

root_coef = 0.7978845608
cubic_coef = 0.044715

swap = [(0, 1), (1, 0)]
axes = ("b", "z", "y", "xl", "xh")
sizes = (2, 4, 4, 2, 2)


def gelu_tanh(values):
    inner = root_coef * (values + cubic_coef * values * values * values)
    return 0.5 * values * (1.0 + jnp.tanh(inner))


def gelu_slope(values):
    tangent = jnp.tanh(root_coef * (values + cubic_coef * values * values * values))
    return 0.5 * (1.0 + tangent) + 0.5 * values * (1.0 - tangent * tangent) * root_coef * (
        1.0 + 3.0 * cubic_coef * values * values
    )


def dot(left, right):
    return jnp.dot(left, right, preferred_element_type=jnp.float32)


def general(left, right, left_dims, right_dims):
    return lax.dot_general(
        left, right, ((left_dims, right_dims), ((), ())), preferred_element_type=jnp.float32
    )


def part(x, index, size, dim):
    return lax.dynamic_slice_in_dim(x, index * size, size, axis=dim)


def ordered(first, mine, other, dim):
    return jnp.where(
        first, jnp.concatenate([mine, other], dim), jnp.concatenate([other, mine], dim)
    )


def number(place):
    result = 0
    for at, size in zip(place, sizes):
        result = result * size + at % size
    return result


def moved(x, step):
    places = itertools.product(*(range(size) for size in sizes))
    return lax.ppermute(x, axes, [(number(p), number(step(*p))) for p in places])


def second(by):
    return lambda b, z, y, xl, xh: (b, z + by * b, y + by * (1 - b), xl, xh)


def third(by):
    return lambda b, z, y, xl, xh: (b, z + by * (1 - b), y + by * b, xl, xh)


def per_device(
    tokens,
    light_in,
    light_out,
    heavy_in,
    heavy_out,
    route_index,
    route_count,
    route_gate,
    cotangent,
):
    core = lax.axis_index("b")
    side = lax.axis_index("xh")
    low = lax.axis_index("xl")
    at_y = lax.axis_index("y")
    at_z = lax.axis_index("z")
    rows, width = tokens.shape
    slots = route_index.shape[1]
    half = slots // 2
    block = heavy_out.shape[1] // 4
    units = heavy_out.shape[0]

    positions = route_index[0]
    live_slots = jnp.arange(slots, dtype=jnp.int32) < route_count[0]
    row_scale = jnp.where(live_slots, route_gate[0], jnp.zeros_like(route_gate[0]))
    own_positions = part(positions, core, half, 0)
    own_scale = part(row_scale, core, half, 0)
    picked = jnp.take(tokens, own_positions, axis=0, mode="clip")
    back = jnp.take(cotangent, own_positions, axis=0, mode="clip").astype(jnp.float32)
    back = (back * own_scale[:, None]).astype(jnp.bfloat16)
    back = lax.all_gather(back, ("xh", "xl", "y", "z", "b"), axis=0, tiled=True)
    back = back.reshape(2, back.shape[0] // 2, width)

    over_side = moved(picked, lambda b, z, y, xl, xh: (b, z, y, xl, xh + 1))
    over_low = moved(picked, lambda b, z, y, xl, xh: (b, z, y, xl + 1, xh))
    over_both = moved(picked, lambda b, z, y, xl, xh: (b, z, y, xl + 1, xh + 1))
    plane = ordered(
        low == 0,
        ordered(side == 0, picked, over_side, 1),
        ordered(side == 0, over_low, over_both, 1),
        0,
    )
    sheet = jnp.concatenate([plane] + [moved(plane, second(-k)) for k in (1, 2, 3)], axis=0)
    after = moved(sheet, third(-1))
    before = moved(sheet, third(1))
    cut = sheet.shape[0] // 2
    facing = jnp.concatenate(
        [moved(after[:cut], third(-1)), moved(before[cut:], third(1))], axis=0
    )
    sheets = (sheet, after, facing, before)

    chip_in = jnp.concatenate([heavy_in, lax.ppermute(heavy_in, "b", swap)], axis=1)
    by_side = heavy_out.reshape(units, 2, 2, block)
    kept = part(by_side, side, 1, 2).reshape(units, 2 * block)
    given = part(by_side, 1 - side, 1, 2).reshape(units, 2 * block)
    got_out = lax.ppermute(given, "xh", swap)
    kept_other = lax.ppermute(kept, "b", swap)
    got_other = lax.ppermute(got_out, "b", swap)
    group_weight = jnp.concatenate([kept, kept_other, got_out, got_other], axis=0)

    sent = part(tokens, core, rows // 2, 0)
    got = lax.ppermute(sent, "xh", swap)
    other = ordered(core == 0, got, lax.ppermute(got, "b", swap), 0)
    whole = ordered(side == 0, tokens, other, 1)
    light_hidden = gelu_tanh(dot(whole, light_in)).astype(jnp.bfloat16)
    mine = dot(light_hidden, part(light_out, core, width, 1))
    theirs = dot(light_hidden, part(light_out, 1 - core, width, 1))
    chip_terms = mine + lax.ppermute(theirs, "b", swap)
    light_share = part(chip_terms, side, block, 1) + lax.ppermute(
        part(chip_terms, 1 - side, block, 1).astype(jnp.bfloat16), "xh", swap
    ).astype(jnp.float32)

    pre_acts, hiddens, acrosses = [], [], []
    for one in sheets:
        pre = dot(one, chip_in)
        hidden = gelu_tanh(pre).astype(jnp.bfloat16)
        pre_acts.append(pre)
        hiddens.append(hidden)
    first_across = lax.ppermute(
        jnp.concatenate([hiddens[0], hiddens[1], hiddens[3]], axis=0), "xh", swap
    )
    last_across = lax.ppermute(hiddens[2], "xh", swap)
    tall = sheet.shape[0]
    across = jnp.concatenate(
        [first_across[: 2 * tall], last_across, first_across[2 * tall :]], axis=0
    )
    hidden = jnp.concatenate(hiddens, axis=0)
    count = hidden.shape[0]
    r = jnp.arange(count, dtype=jnp.int32)
    r_slot, r_z, r_y, r_low = r % half, r // half % 4, r // (4 * half) % 4, r // (16 * half)
    turn_z, turn_y = (r_z - at_z) % 4, (r_y - at_y) % 4
    inner = r_low * half + r_slot
    place = jnp.where(core == 0, turn_z * 4 + turn_y, turn_y * 4 + turn_z) * (2 * half) + inner
    place_other = (
        jnp.where(core == 0, turn_y * 4 + turn_z, turn_z * 4 + turn_y) * (2 * half) + inner
    )
    choice = (place[:, None] == r[None, :]).astype(jnp.bfloat16)
    group_hidden = dot(choice, jnp.concatenate([hidden, across], axis=1)).astype(jnp.bfloat16)
    partial_terms = dot(group_hidden, group_weight).astype(jnp.bfloat16)
    arrived = lax.all_to_all(partial_terms, ("xl", "y", "z"), 0, 0, tiled=True)
    homed = arrived.reshape(-1, half, 2 * block).astype(jnp.float32).sum(axis=0)
    swapped = lax.ppermute(part(homed, 1 - core, block, 1), "b", swap)
    heavy_share = ordered(core == 0, part(homed, core, block, 1), swapped, 0) * row_scale[:, None]
    naming = (jnp.arange(rows, dtype=jnp.int32)[:, None] == positions[None, :]).astype(jnp.float32)
    spread = jnp.dot(
        naming, heavy_share, precision=lax.Precision.HIGHEST, preferred_element_type=jnp.float32
    )
    mixed = (light_share + spread).astype(jnp.bfloat16)

    pre_act = jnp.concatenate(pre_acts, axis=0)
    pre_rows = jnp.dot(
        choice.astype(jnp.float32),
        pre_act,
        precision=lax.Precision.HIGHEST,
        preferred_element_type=jnp.float32,
    )

    def both_cores(own, theirs):
        pieces = [own.reshape(-1, 1, half, units), theirs.reshape(-1, 1, half, units)]
        return ordered(core == 0, pieces[0], pieces[1], 1).reshape(2 * count, units)

    pre_all = both_cores(pre_rows[:, :units], lax.ppermute(pre_rows[:, units:], "b", swap))
    hidden_all = gelu_tanh(pre_all).astype(jnp.bfloat16)
    slope = general(back[0], heavy_out[:, :width], (1,), (1,)) + general(
        back[1], heavy_out[:, width:], (1,), (1,)
    )
    slope = (slope * gelu_slope(pre_all)).astype(jnp.bfloat16)
    grad_out = jnp.concatenate(
        [general(hidden_all, back[k], (0,), (0,)) for k in (0, 1)], axis=1
    ).astype(jnp.bfloat16)
    places = jnp.stack([place, place_other + count])
    places = jnp.where(core == 0, places, places[::-1])
    places = places.reshape(2, -1, half).swapaxes(0, 1).reshape(-1)
    wide = jnp.arange(2 * count, dtype=jnp.int32)
    back_choice = (wide[:, None] == places[None, :]).astype(jnp.bfloat16)
    slope_rows = dot(back_choice, slope).astype(jnp.bfloat16)
    theirs_sheets = [lax.ppermute(one, "b", swap) for one in sheets]
    picked_all = jnp.concatenate(list(sheets) + theirs_sheets, axis=0)
    grad_in = general(picked_all, slope_rows, (0,), (0,)).astype(jnp.bfloat16)
    return (mixed, grad_in, grad_out)


def solution(mesh):
    split = Mesh(mesh.devices.reshape(*sizes), axes)
    seq = ("z", "y", "xl")
    units = axes
    in_specs = (
        P(seq, "xh"),
        P(None, ("b", "xh")),
        P(("b", "xh"), None),
        P(None, units),
        P(units, None),
        P(seq, None),
        P(seq),
        P(seq, None),
        P(seq, "xh"),
    )
    out_specs = (
        P(seq, ("b", "xh")),
        P(None, units),
        P(units, None),
    )
    return jax.shard_map(
        per_device, mesh=split, in_specs=in_specs, out_specs=out_specs, check_vma=False
    )
```

```python
import itertools

import jax
import jax.numpy as jnp
from jax import lax
from jax.experimental import pallas as pl
from jax.sharding import Mesh, PartitionSpec as P


root_coef = 0.7978845608
cubic_coef = 0.044715

swap = [(0, 1), (1, 0)]
axes = ("b", "z", "y", "xl", "xh")
sizes = (2, 4, 4, 2, 2)


def gelu_tanh(values):
    inner = root_coef * (values + cubic_coef * values * values * values)
    return 0.5 * values * (1.0 + jnp.tanh(inner))


def gelu_slope(values):
    tangent = jnp.tanh(root_coef * (values + cubic_coef * values * values * values))
    return 0.5 * (1.0 + tangent) + 0.5 * values * (1.0 - tangent * tangent) * root_coef * (
        1.0 + 3.0 * cubic_coef * values * values
    )


def dot(left, right):
    return jnp.dot(left, right, preferred_element_type=jnp.float32)


def general(left, right, left_dims, right_dims):
    return lax.dot_general(
        left, right, ((left_dims, right_dims), ((), ())), preferred_element_type=jnp.float32
    )


def part(x, index, size, dim):
    return lax.dynamic_slice_in_dim(x, index * size, size, axis=dim)


def ordered(first, mine, other, dim):
    return jnp.where(
        first, jnp.concatenate([mine, other], dim), jnp.concatenate([other, mine], dim)
    )


def number(place):
    result = 0
    for at, size in zip(place, sizes):
        result = result * size + at % size
    return result


def moved(x, step):
    places = itertools.product(*(range(size) for size in sizes))
    return lax.ppermute(x, axes, [(number(p), number(step(*p))) for p in places])


def second(by):
    return lambda b, z, y, xl, xh: (b, z + by * b, y + by * (1 - b), xl, xh)


def third(by):
    return lambda b, z, y, xl, xh: (b, z + by * (1 - b), y + by * b, xl, xh)


def rows_product(left, tiles):
    return lax.dot_general(
        left, tiles, (((0,), (0,)), ((), ())), preferred_element_type=jnp.float32
    )


def grad_out_of(hidden, back, tile=512):
    sides, rows, width = back.shape
    units = hidden.shape[1]
    per_side = width // tile

    def kernel(hidden_ref, back_ref, out_ref):
        out_ref[...] = rows_product(hidden_ref[...], back_ref[0]).astype(out_ref.dtype)

    return pl.pallas_call(
        kernel,
        grid=(sides * per_side,),
        in_specs=[
            pl.BlockSpec((rows, units), lambda i: (0, 0)),
            pl.BlockSpec((1, rows, tile), lambda i: (i // per_side, 0, i % per_side)),
        ],
        out_specs=pl.BlockSpec((units, tile), lambda i: (0, i)),
        out_shape=jax.ShapeDtypeStruct((units, sides * width), jnp.bfloat16),
        cost_estimate=pl.CostEstimate(
            flops=2 * rows * units * sides * width,
            bytes_accessed=2 * (sides * rows * width + units * sides * width),
            transcendentals=0,
        ),
    )(hidden, back)


def grad_in_of(sheets, slope, tile=512):
    tall, features = sheets[0].shape
    rows, units = slope.shape

    def kernel(*refs):
        slope_ref, out_ref = refs[-2:]
        tiles = jnp.concatenate([ref[...] for ref in refs[:-2]], axis=0)
        out_ref[...] = rows_product(slope_ref[...], tiles).T.astype(out_ref.dtype)

    return pl.pallas_call(
        kernel,
        grid=(features // tile,),
        in_specs=[pl.BlockSpec((tall, tile), lambda i: (0, i)) for _ in sheets]
        + [pl.BlockSpec((rows, units), lambda i: (0, 0))],
        out_specs=pl.BlockSpec((tile, units), lambda i: (i, 0)),
        out_shape=jax.ShapeDtypeStruct((features, units), jnp.bfloat16),
        cost_estimate=pl.CostEstimate(
            flops=2 * rows * units * features,
            bytes_accessed=2 * (rows * features + units * features),
            transcendentals=0,
        ),
    )(*sheets, slope)


def per_device(
    tokens,
    light_in,
    light_out,
    heavy_in,
    heavy_out,
    route_index,
    route_count,
    route_gate,
    cotangent,
):
    core = lax.axis_index("b")
    side = lax.axis_index("xh")
    low = lax.axis_index("xl")
    at_y = lax.axis_index("y")
    at_z = lax.axis_index("z")
    rows, width = tokens.shape
    slots = route_index.shape[1]
    half = slots // 2
    block = heavy_out.shape[1] // 4
    units = heavy_out.shape[0]

    positions = route_index[0]
    live_slots = jnp.arange(slots, dtype=jnp.int32) < route_count[0]
    row_scale = jnp.where(live_slots, route_gate[0], jnp.zeros_like(route_gate[0]))
    own_positions = part(positions, core, half, 0)
    own_scale = part(row_scale, core, half, 0)
    picked = jnp.take(tokens, own_positions, axis=0, mode="clip")
    picked, later_positions = lax.optimization_barrier((picked, own_positions))
    back = jnp.take(cotangent, later_positions, axis=0, mode="clip").astype(jnp.float32)
    back = (back * own_scale[:, None]).astype(jnp.bfloat16)
    back = lax.all_gather(back, ("xh", "xl", "y", "z", "b"), axis=0, tiled=True)
    back = back.reshape(2, back.shape[0] // 2, width)

    over_side = moved(picked, lambda b, z, y, xl, xh: (b, z, y, xl, xh + 1))
    over_low = moved(picked, lambda b, z, y, xl, xh: (b, z, y, xl + 1, xh))
    over_both = moved(picked, lambda b, z, y, xl, xh: (b, z, y, xl + 1, xh + 1))
    plane = ordered(
        low == 0,
        ordered(side == 0, picked, over_side, 1),
        ordered(side == 0, over_low, over_both, 1),
        0,
    )
    plane, later_tokens = lax.optimization_barrier((plane, tokens))
    sheet = jnp.concatenate([plane] + [moved(plane, second(-k)) for k in (1, 2, 3)], axis=0)
    sheet, later_out = lax.optimization_barrier((sheet, heavy_out))
    after = moved(sheet, third(-1))
    before = moved(sheet, third(1))
    cut = sheet.shape[0] // 2
    facing = [moved(after[:cut], third(-1)), moved(before[cut:], third(1))]
    facing = jnp.concatenate(facing, axis=0)
    sheets = (sheet, after, facing, before)

    chip_in = jnp.concatenate([heavy_in, lax.ppermute(heavy_in, "b", swap)], axis=1)
    kept = jnp.concatenate([part(later_out, 2 * k + side, block, 1) for k in (0, 1)], axis=1)
    given = [part(later_out, 2 * k + 1 - side, block, 1) for k in (0, 1)]
    given = jnp.concatenate(given, axis=1)
    got_out = lax.ppermute(given, "xh", swap)
    kept_other = lax.ppermute(kept, "b", swap)
    got_other = lax.ppermute(got_out, "b", swap)
    group_weight = jnp.concatenate([kept, kept_other, got_out, got_other], axis=0)

    sent = part(later_tokens, core, rows // 2, 0)
    got = lax.ppermute(sent, "xh", swap)
    other = ordered(core == 0, got, lax.ppermute(got, "b", swap), 0)
    whole = ordered(side == 0, tokens, other, 1)
    light_hidden = gelu_tanh(dot(whole, light_in)).astype(jnp.bfloat16)
    theirs = dot(light_hidden, part(light_out, 1 - core, width, 1))
    mine = dot(light_hidden, part(light_out, core, width, 1))
    chip_terms = mine + lax.ppermute(theirs, "b", swap)
    light_kept = part(chip_terms, side, block, 1)
    light_given = part(chip_terms, 1 - side, block, 1).astype(jnp.bfloat16)

    pre_acts = []
    for name, one in zip(("pre_own", "pre_near", "pre_facing", "pre_near"), sheets):
        pre = dot(one, chip_in)
        if name != "pre_facing":
            pre = lax.optimization_barrier(pre)
        pre_acts.append(pre)
    tall = sheet.shape[0]
    early = jnp.concatenate([pre_acts[1], pre_acts[3], pre_acts[0]], axis=0)
    early = gelu_tanh(early).astype(jnp.bfloat16)
    early = jnp.concatenate([early, lax.ppermute(early, "xh", swap)], axis=1)
    late = gelu_tanh(pre_acts[2]).astype(jnp.bfloat16)
    across = lax.ppermute(late, "xh", swap)
    late = jnp.concatenate([late, across], axis=1)
    near = dot(early[: 2 * tall], group_weight).astype(jnp.bfloat16)
    far = dot(late, group_weight).astype(jnp.bfloat16)
    light_got = lax.ppermute(light_given, "xh", swap)
    light_share = light_kept + light_got.astype(jnp.float32)
    own = dot(early[2 * tall :], group_weight)
    from_before = moved(near[:tall], third(1))
    from_after = moved(near[tall:], third(-1))
    from_facing = moved(far, third(2))
    for one in (from_before, from_after, from_facing):
        own = own + one.astype(jnp.float32)
    strip = plane.shape[0]
    leaving = own.astype(jnp.bfloat16)
    total = own[:strip]
    strips = [moved(leaving[k * strip : (k + 1) * strip], second(k)) for k in (1, 2, 3)]
    for one in strips:
        total = total + one.astype(jnp.float32)
    count = 4 * tall
    r = jnp.arange(count, dtype=jnp.int32)
    r_slot, r_z, r_y, r_low = r % half, r // half % 4, r // (4 * half) % 4, r // (16 * half)
    turn_z, turn_y = (r_z - at_z) % 4, (r_y - at_y) % 4
    inner = r_low * half + r_slot
    place = jnp.where(core == 0, turn_z * 4 + turn_y, turn_y * 4 + turn_z) * (2 * half) + inner
    place_other = (
        jnp.where(core == 0, turn_y * 4 + turn_z, turn_z * 4 + turn_y) * (2 * half) + inner
    )
    choice = (place[:, None] == r[None, :]).astype(jnp.bfloat16)

    pre_act = jnp.concatenate(pre_acts, axis=0)
    pre_rows = jnp.dot(
        choice.astype(jnp.float32),
        pre_act,
        precision=lax.Precision.HIGHEST,
        preferred_element_type=jnp.float32,
    )

    def both_cores(own, theirs):
        pieces = [own.reshape(-1, 1, half, units), theirs.reshape(-1, 1, half, units)]
        return ordered(core == 0, pieces[0], pieces[1], 1).reshape(2 * count, units)

    pre_all = both_cores(pre_rows[:, :units], lax.ppermute(pre_rows[:, units:], "b", swap))
    hidden_all = gelu_tanh(pre_all).astype(jnp.bfloat16)
    slope = general(back[0], heavy_out[:, :width], (1,), (1,)) + general(
        back[1], heavy_out[:, width:], (1,), (1,)
    )
    slope = (slope * gelu_slope(pre_all)).astype(jnp.bfloat16)
    grad_out = grad_out_of(hidden_all, back)
    places = jnp.stack([place, place_other + count])
    places = jnp.where(core == 0, places, places[::-1])
    places = places.reshape(2, -1, half).swapaxes(0, 1).reshape(-1)
    wide = jnp.arange(2 * count, dtype=jnp.int32)
    back_choice = (wide[:, None] == places[None, :]).astype(jnp.bfloat16)
    slope_rows = dot(back_choice, slope).astype(jnp.bfloat16)
    total, slope_rows, grad_out = lax.optimization_barrier((total, slope_rows, grad_out))
    homed = part(total, low, half, 0) + lax.ppermute(
        part(total, 1 - low, half, 0).astype(jnp.bfloat16), "xl", swap
    ).astype(jnp.float32)
    theirs_sheets = [lax.ppermute(one, "b", swap) for one in sheets]
    grad_in = grad_in_of(list(sheets) + theirs_sheets, slope_rows)
    swapped = lax.ppermute(part(homed, 1 - core, block, 1), "b", swap)
    heavy_share = ordered(core == 0, part(homed, core, block, 1), swapped, 0) * row_scale[:, None]
    naming = (jnp.arange(rows, dtype=jnp.int32)[:, None] == positions[None, :]).astype(jnp.float32)
    spread = jnp.dot(
        naming, heavy_share, precision=lax.Precision.HIGHEST, preferred_element_type=jnp.float32
    )
    mixed = (light_share + spread).astype(jnp.bfloat16)


    return (mixed, grad_in, grad_out)


def solution(mesh):
    split = Mesh(mesh.devices.reshape(*sizes), axes)
    seq = ("z", "y", "xl")
    units = axes
    in_specs = (
        P(seq, "xh"),
        P(None, ("b", "xh")),
        P(("b", "xh"), None),
        P(None, units),
        P(units, None),
        P(seq, None),
        P(seq),
        P(seq, None),
        P(seq, "xh"),
    )
    out_specs = (
        P(seq, ("b", "xh")),
        P(None, units),
        P(units, None),
    )

    return jax.shard_map(
        per_device, mesh=split, in_specs=in_specs, out_specs=out_specs, check_vma=False
    )
```

```python
import itertools

import jax
import jax.numpy as jnp
from jax import lax
from jax.experimental import pallas as pl
from jax.experimental.pallas import tpu as pltpu
from jax.sharding import Mesh, PartitionSpec as P


root_coef = 0.7978845608
cubic_coef = 0.044715

swap = [(0, 1), (1, 0)]
axes = ("b", "z", "y", "xl", "xh")
sizes = (2, 4, 4, 2, 2)


def gelu_tanh(values):
    inner = root_coef * (values + cubic_coef * values * values * values)
    return 0.5 * values * (1.0 + jnp.tanh(inner))


def gelu_slope(values):
    tangent = jnp.tanh(root_coef * (values + cubic_coef * values * values * values))
    return 0.5 * (1.0 + tangent) + 0.5 * values * (1.0 - tangent * tangent) * root_coef * (
        1.0 + 3.0 * cubic_coef * values * values
    )


def dot(left, right):
    return jnp.dot(left, right, preferred_element_type=jnp.float32)


def general(left, right, left_dims, right_dims):
    return lax.dot_general(
        left, right, ((left_dims, right_dims), ((), ())), preferred_element_type=jnp.float32
    )


def part(x, index, size, dim):
    return lax.dynamic_slice_in_dim(x, index * size, size, axis=dim)


def ordered(first, mine, other, dim):
    return jnp.where(
        first, jnp.concatenate([mine, other], dim), jnp.concatenate([other, mine], dim)
    )


def number(place):
    result = 0
    for at, size in zip(place, sizes):
        result = result * size + at % size
    return result


def moved(x, step):
    places = itertools.product(*(range(size) for size in sizes))
    return lax.ppermute(x, axes, [(number(p), number(step(*p))) for p in places])


def second(by):
    return lambda b, z, y, xl, xh: (b, z + by * b, y + by * (1 - b), xl, xh)


def third(by):
    return lambda b, z, y, xl, xh: (b, z + by * (1 - b), y + by * b, xl, xh)


def grad_out_of(pre, weight, back, places, tile=512):
    rows, features = back.shape
    units = pre.shape[1]
    last = features // tile - 1

    def kernel(pre_ref, weight_ref, back_ref, places_ref, out_ref, slope_ref, hidden, total):
        step = pl.program_id(0)

        @pl.when(step == 0)
        def _():
            hidden[...] = gelu_tanh(pre_ref[...]).T.astype(hidden.dtype)
            total[...] = jnp.zeros_like(total)

        tiles = back_ref[...]
        out_ref[...] = dot(hidden[...], tiles).astype(out_ref.dtype)
        total[...] += general(tiles, weight_ref[...], (1,), (1,))

        @pl.when(step == last)
        def _():
            slope = (total[...] * gelu_slope(pre_ref[...])).T.astype(slope_ref.dtype)
            for at in range(0, rows, 256):
                target = at + lax.broadcasted_iota(jnp.int32, (256, rows), 0)
                moves = (target == places_ref[...]).astype(jnp.float32).astype(slope.dtype)
                slope_ref[:, at : at + 256] = general(slope, moves, (1,), (1,)).astype(
                    slope_ref.dtype
                )

    return pl.pallas_call(
        kernel,
        grid=(last + 1,),
        in_specs=[
            pl.BlockSpec((rows, units), lambda i: (0, 0)),
            pl.BlockSpec((units, tile), lambda i: (0, i)),
            pl.BlockSpec((rows, tile), lambda i: (0, i)),
            pl.BlockSpec((1, rows), lambda i: (0, 0)),
        ],
        out_specs=[
            pl.BlockSpec((units, tile), lambda i: (0, i)),
            pl.BlockSpec((units, rows), lambda i: (0, 0)),
        ],
        out_shape=[
            jax.ShapeDtypeStruct((units, features), jnp.bfloat16),
            jax.ShapeDtypeStruct((units, rows), jnp.bfloat16),
        ],
        scratch_shapes=[
            pltpu.VMEM((units, rows), jnp.bfloat16),
            pltpu.VMEM((rows, units), jnp.float32),
        ],
        cost_estimate=pl.CostEstimate(
            flops=4 * rows * units * features,
            bytes_accessed=2 * (rows * features + 2 * units * features),
            transcendentals=0,
        ),
    )(pre, weight, back, places)


def grad_in_of(sheets, slope, tile=512):
    tall, features = sheets[0].shape
    units, rows = slope.shape

    def kernel(*refs):
        slope_ref, out_ref = refs[-2:]
        tiles = jnp.concatenate([ref[...] for ref in refs[:-2]], axis=0)
        out_ref[...] = dot(slope_ref[...], tiles).T.astype(out_ref.dtype)

    return pl.pallas_call(
        kernel,
        grid=(features // tile,),
        in_specs=[pl.BlockSpec((tall, tile), lambda i: (0, i)) for _ in sheets]
        + [pl.BlockSpec((units, rows), lambda i: (0, 0))],
        out_specs=pl.BlockSpec((tile, units), lambda i: (i, 0)),
        out_shape=jax.ShapeDtypeStruct((features, units), jnp.bfloat16),
        cost_estimate=pl.CostEstimate(
            flops=2 * rows * units * features,
            bytes_accessed=2 * (rows * features + units * features),
            transcendentals=0,
        ),
    )(*sheets, slope)


def per_device(
    tokens,
    light_in,
    light_out,
    heavy_in,
    heavy_out,
    route_index,
    route_count,
    route_gate,
    cotangent,
):
    core = lax.axis_index("b")
    side = lax.axis_index("xh")
    low = lax.axis_index("xl")
    at_y = lax.axis_index("y")
    at_z = lax.axis_index("z")
    rows, width = tokens.shape
    slots = route_index.shape[1]
    half = slots // 2
    block = heavy_out.shape[1] // 4
    units = heavy_out.shape[0]

    positions = route_index[0]
    live_slots = jnp.arange(slots, dtype=jnp.int32) < route_count[0]
    row_scale = jnp.where(live_slots, route_gate[0], jnp.zeros_like(route_gate[0]))
    own_positions = part(positions, core, half, 0)
    own_scale = part(row_scale, core, half, 0)
    back = jnp.take(cotangent, own_positions, axis=0, mode="clip").astype(jnp.float32)
    back = (back * own_scale[:, None]).astype(jnp.bfloat16)
    both = jnp.concatenate([jnp.take(tokens, own_positions, axis=0, mode="clip"), back], axis=0)

    over_side = moved(both, lambda b, z, y, xl, xh: (b, z, y, xl, xh + 1))
    over_low = moved(both, lambda b, z, y, xl, xh: (b, z, y, xl + 1, xh))
    over_both = moved(both, lambda b, z, y, xl, xh: (b, z, y, xl + 1, xh + 1))

    mine = ordered(side == 0, both, over_side, 1)
    other = ordered(side == 0, over_low, over_both, 1)
    plane = ordered(low == 0, mine[:half], other[:half], 0)
    back = ordered(low == 0, mine[half:], other[half:], 0)
    back = lax.all_gather(back, ("z", "y", "b"), axis=0, tiled=True)
    plane, later_tokens, later_out = lax.optimization_barrier((plane, tokens, heavy_out))
    sheet = [plane] + [moved(plane, second(-k)) for k in (1, 2, 3)]
    sheet = jnp.concatenate(sheet, axis=0)
    after = moved(sheet, third(-1))
    before = moved(sheet, third(1))
    cut = sheet.shape[0] // 2
    facing = [moved(after[:cut], third(-1)), moved(before[cut:], third(1))]
    facing = jnp.concatenate(facing, axis=0)
    sheets = (sheet, after, facing, before)

    chip_in = jnp.concatenate([heavy_in, lax.ppermute(heavy_in, "b", swap)], axis=1)
    kept = jnp.concatenate([part(later_out, 2 * k + side, block, 1) for k in (0, 1)], axis=1)
    given = [part(later_out, 2 * k + 1 - side, block, 1) for k in (0, 1)]
    given = jnp.concatenate(given, axis=1)
    got_out = lax.ppermute(given, "xh", swap)
    kept_other = lax.ppermute(kept, "b", swap)
    got_other = lax.ppermute(got_out, "b", swap)
    group_weight = jnp.concatenate([kept, kept_other, got_out, got_other], axis=0)

    sent = part(later_tokens, core, rows // 2, 0)
    got = lax.ppermute(sent, "xh", swap)
    other = ordered(core == 0, got, lax.ppermute(got, "b", swap), 0)
    whole = ordered(side == 0, tokens, other, 1)
    light_hidden = gelu_tanh(dot(whole, light_in)).astype(jnp.bfloat16)
    theirs = dot(light_hidden, part(light_out, 1 - core, width, 1))
    mine = dot(light_hidden, part(light_out, core, width, 1))
    chip_terms = mine + lax.ppermute(theirs, "b", swap)
    light_kept = part(chip_terms, side, block, 1)
    light_given = part(chip_terms, 1 - side, block, 1).astype(jnp.bfloat16)

    pre_acts = []
    for name, one in zip(("pre_own", "pre_near", "pre_facing", "pre_near"), sheets):
        pre = dot(one, chip_in)
        if name != "pre_facing":
            pre = lax.optimization_barrier(pre)
        pre_acts.append(pre)
    tall = sheet.shape[0]
    early = jnp.concatenate([pre_acts[1], pre_acts[3], pre_acts[0]], axis=0)
    early = gelu_tanh(early).astype(jnp.bfloat16)
    early = jnp.concatenate([early, lax.ppermute(early, "xh", swap)], axis=1)
    late = gelu_tanh(pre_acts[2]).astype(jnp.bfloat16)
    across = lax.ppermute(late, "xh", swap)
    late = jnp.concatenate([late, across], axis=1)
    near = dot(early[: 2 * tall], group_weight).astype(jnp.bfloat16)
    far = dot(late, group_weight).astype(jnp.bfloat16)
    light_got = lax.ppermute(light_given, "xh", swap)
    light_share = light_kept + light_got.astype(jnp.float32)
    own = dot(early[2 * tall :], group_weight)
    from_before = moved(near[:tall], third(1))
    from_after = moved(near[tall:], third(-1))
    from_facing = moved(far, third(2))
    for one in (from_before, from_after, from_facing):
        own = own + one.astype(jnp.float32)
    strip = plane.shape[0]
    leaving = own.astype(jnp.bfloat16)
    total = own[:strip]
    strips = [moved(leaving[k * strip : (k + 1) * strip], second(k)) for k in (1, 2, 3)]
    for one in strips:
        total = total + one.astype(jnp.float32)
    count = 4 * tall
    r = jnp.arange(count, dtype=jnp.int32)
    inner, r_y, r_z = r % strip, r // strip % 4, r // tall
    turn_z, turn_y = (r_z - at_z) % 4, (r_y - at_y) % 4
    place = jnp.where(core == 0, turn_z * 4 + turn_y, turn_y * 4 + turn_z) * strip + inner
    place_other = jnp.where(core == 0, turn_y * 4 + turn_z, turn_z * 4 + turn_y) * strip + inner
    choice = (place[:, None] == r[None, :]).astype(jnp.bfloat16)

    pre_act = jnp.concatenate(pre_acts, axis=0)
    pre_rows = jnp.dot(
        choice.astype(jnp.float32),
        pre_act,
        precision=lax.Precision.HIGHEST,
        preferred_element_type=jnp.float32,
    )

    def both_cores(own, theirs):
        pieces = [own.reshape(-1, 1, strip, units), theirs.reshape(-1, 1, strip, units)]
        return ordered(core == 0, pieces[0], pieces[1], 1).reshape(2 * count, units)

    pre_all = both_cores(pre_rows[:, :units], lax.ppermute(pre_rows[:, units:], "b", swap))
    places = jnp.where(
        core == 0,
        jnp.stack([place, place_other + count]),
        jnp.stack([place_other + count, place]),
    )
    places = places.reshape(2, -1, strip).swapaxes(0, 1).reshape(1, -1)
    grad_out, slope_rows = grad_out_of(pre_all, heavy_out, back, places)
    total, slope_rows, grad_out = lax.optimization_barrier((total, slope_rows, grad_out))
    homed = part(total, low, half, 0) + lax.ppermute(
        part(total, 1 - low, half, 0).astype(jnp.bfloat16), "xl", swap
    ).astype(jnp.float32)
    theirs_sheets = [lax.ppermute(one, "b", swap) for one in sheets]
    grad_in = grad_in_of(list(sheets) + theirs_sheets, slope_rows)
    swapped = lax.ppermute(part(homed, 1 - core, block, 1), "b", swap)
    heavy_share = ordered(core == 0, part(homed, core, block, 1), swapped, 0) * row_scale[:, None]
    naming = (jnp.arange(rows, dtype=jnp.int32)[:, None] == positions[None, :]).astype(jnp.float32)
    spread = jnp.dot(
        naming, heavy_share, precision=lax.Precision.HIGHEST, preferred_element_type=jnp.float32
    )
    mixed = (light_share + spread).astype(jnp.bfloat16)


    return (mixed, grad_in, grad_out)


def solution(mesh):
    split = Mesh(mesh.devices.reshape(*sizes), axes)
    seq = ("z", "y", "xl")
    units = axes
    in_specs = (
        P(seq, "xh"),
        P(None, ("b", "xh")),
        P(("b", "xh"), None),
        P(None, units),
        P(units, None),
        P(seq, None),
        P(seq),
        P(seq, None),
        P(seq, "xh"),
    )
    out_specs = (
        P(seq, ("b", "xh")),
        P(None, units),
        P(units, None),
    )

    return jax.shard_map(
        per_device, mesh=split, in_specs=in_specs, out_specs=out_specs, check_vma=False
    )
```

```python
import itertools

import jax
import jax.numpy as jnp
from jax import lax
from jax.experimental import pallas as pl
from jax.experimental.pallas import tpu as pltpu
from jax.sharding import Mesh, PartitionSpec as P


root_coef = 0.7978845608
cubic_coef = 0.044715

swap = [(0, 1), (1, 0)]
axes = ("b", "z", "y", "xl", "xh")
grant = 20 << 20
whole = pl.BlockSpec(memory_space=pltpu.VMEM)
sizes = (2, 4, 4, 2, 2)


def gelu_tanh(values):
    inner = root_coef * (values + cubic_coef * values * values * values)
    return 0.5 * values * (1.0 + jnp.tanh(inner))


def gelu_slope(values):
    tangent = jnp.tanh(root_coef * (values + cubic_coef * values * values * values))
    return 0.5 * (1.0 + tangent) + 0.5 * values * (1.0 - tangent * tangent) * root_coef * (
        1.0 + 3.0 * cubic_coef * values * values
    )


def dot(left, right):
    return jnp.dot(left, right, preferred_element_type=jnp.float32)


def general(left, right, left_dims, right_dims):
    return lax.dot_general(
        left, right, ((left_dims, right_dims), ((), ())), preferred_element_type=jnp.float32
    )


def part(x, index, size, dim):
    return lax.dynamic_slice_in_dim(x, index * size, size, axis=dim)


def ordered(first, mine, other, dim):
    return jnp.where(
        first, jnp.concatenate([mine, other], dim), jnp.concatenate([other, mine], dim)
    )


def number(place):
    result = 0
    for at, size in zip(place, sizes):
        result = result * size + at % size
    return result


def moved(x, step):
    places = itertools.product(*(range(size) for size in sizes))
    return lax.ppermute(x, axes, [(number(p), number(step(*p))) for p in places])


def second(by):
    return lambda b, z, y, xl, xh: (b, z + by * b, y + by * (1 - b), xl, xh)


def third(by):
    return lambda b, z, y, xl, xh: (b, z + by * (1 - b), y + by * b, xl, xh)


def grad_out_of(pre, weight, back, places, tile=512):
    rows, features = back.shape
    units = pre.shape[1]

    def kernel(pre_ref, weight_ref, back_ref, places_ref, out_ref, slope_ref, total):
        hidden = gelu_tanh(pre_ref[...]).T.astype(jnp.bfloat16)
        for at in range(0, features, tile):
            tiles = back_ref[:, at : at + tile]
            out_ref[:, at : at + tile] = dot(hidden, tiles).astype(out_ref.dtype)
            term = general(tiles, weight_ref[:, at : at + tile], (1,), (1,))
            total[...] = total[...] + term if at else term
        slope = (total[...] * gelu_slope(pre_ref[...])).T.astype(slope_ref.dtype)
        for at in range(0, rows, 256):
            target = at + lax.broadcasted_iota(jnp.int32, (256, rows), 0)
            moves = (target == places_ref[...]).astype(jnp.float32).astype(slope.dtype)
            slope_ref[:, at : at + 256] = general(slope, moves, (1,), (1,)).astype(slope_ref.dtype)

    return pl.pallas_call(
        kernel,
        in_specs=[whole] * 4,
        out_specs=[whole] * 2,
        out_shape=[
            jax.ShapeDtypeStruct((units, features), jnp.bfloat16),
            jax.ShapeDtypeStruct((units, rows), jnp.bfloat16),
        ],
        scratch_shapes=[pltpu.VMEM((rows, units), jnp.float32)],
        compiler_params=pltpu.CompilerParams(vmem_limit_bytes=grant),
        cost_estimate=pl.CostEstimate(
            flops=4 * rows * units * features,
            bytes_accessed=2 * (rows * features + 2 * units * features),
            transcendentals=0,
        ),
    )(pre, weight, back, places)


def grad_in_of(sheets, slope, tile=512):
    features = sheets[0].shape[1]
    units, rows = slope.shape

    def kernel(*refs):
        slope_ref, out_ref = refs[-2:]
        for at in range(0, features, tile):
            tiles = jnp.concatenate([ref[:, at : at + tile] for ref in refs[:-2]], axis=0)
            out_ref[at : at + tile, :] = dot(slope_ref[...], tiles).T.astype(out_ref.dtype)

    return pl.pallas_call(
        kernel,
        in_specs=[whole] * (len(sheets) + 1),
        out_specs=whole,
        out_shape=jax.ShapeDtypeStruct((features, units), jnp.bfloat16),
        compiler_params=pltpu.CompilerParams(vmem_limit_bytes=grant),
        cost_estimate=pl.CostEstimate(
            flops=2 * rows * units * features,
            bytes_accessed=2 * (rows * features + units * features),
            transcendentals=0,
        ),
    )(*sheets, slope)


def per_device(
    tokens,
    light_in,
    light_out,
    heavy_in,
    heavy_out,
    route_index,
    route_count,
    route_gate,
    cotangent,
):
    core = lax.axis_index("b")
    side = lax.axis_index("xh")
    low = lax.axis_index("xl")
    at_y = lax.axis_index("y")
    at_z = lax.axis_index("z")
    rows, width = tokens.shape
    slots = route_index.shape[1]
    half = slots // 2
    block = heavy_out.shape[1] // 4
    units = heavy_out.shape[0]

    positions = route_index[0]
    live_slots = jnp.arange(slots, dtype=jnp.int32) < route_count[0]
    row_scale = jnp.where(live_slots, route_gate[0], jnp.zeros_like(route_gate[0]))
    own_positions = part(positions, core, half, 0)
    own_scale = part(row_scale, core, half, 0)
    back = jnp.take(cotangent, own_positions, axis=0, mode="clip").astype(jnp.float32)
    back = (back * own_scale[:, None]).astype(jnp.bfloat16)
    both = jnp.concatenate([jnp.take(tokens, own_positions, axis=0, mode="clip"), back], axis=0)

    over_side = moved(both, lambda b, z, y, xl, xh: (b, z, y, xl, xh + 1))
    over_low = moved(both, lambda b, z, y, xl, xh: (b, z, y, xl + 1, xh))
    over_both = moved(both, lambda b, z, y, xl, xh: (b, z, y, xl + 1, xh + 1))

    mine = ordered(side == 0, both, over_side, 1)
    other = ordered(side == 0, over_low, over_both, 1)
    plane = ordered(low == 0, mine[:half], other[:half], 0)
    back = ordered(low == 0, mine[half:], other[half:], 0)
    back = lax.all_gather(back, ("z", "y", "b"), axis=0, tiled=True)
    plane, later_tokens, later_out = lax.optimization_barrier((plane, tokens, heavy_out))
    sheet = [plane] + [moved(plane, second(-k)) for k in (1, 2, 3)]
    sheet = jnp.concatenate(sheet, axis=0)
    after = moved(sheet, third(-1))
    before = moved(sheet, third(1))
    cut = sheet.shape[0] // 2
    facing = [moved(after[:cut], third(-1)), moved(before[cut:], third(1))]
    facing = jnp.concatenate(facing, axis=0)
    sheets = (sheet, after, facing, before)

    chip_in = jnp.concatenate([heavy_in, lax.ppermute(heavy_in, "b", swap)], axis=1)
    kept = jnp.concatenate([part(later_out, 2 * k + side, block, 1) for k in (0, 1)], axis=1)
    given = [part(later_out, 2 * k + 1 - side, block, 1) for k in (0, 1)]
    given = jnp.concatenate(given, axis=1)
    got_out = lax.ppermute(given, "xh", swap)
    kept_other = lax.ppermute(kept, "b", swap)
    got_other = lax.ppermute(got_out, "b", swap)
    group_weight = jnp.concatenate([kept, kept_other, got_out, got_other], axis=0)

    sent = part(later_tokens, core, rows // 2, 0)
    got = lax.ppermute(sent, "xh", swap)
    got_tokens = lax.ppermute(got, "b", swap)
    other = ordered(core == 0, got, got_tokens, 0)
    whole = ordered(side == 0, tokens, other, 1)
    light_hidden = gelu_tanh(dot(whole, light_in)).astype(jnp.bfloat16)
    theirs = dot(light_hidden, part(light_out, 1 - core, width, 1))
    mine = dot(light_hidden, part(light_out, core, width, 1))
    chip_terms = mine + lax.ppermute(theirs, "b", swap)
    light_kept = part(chip_terms, side, block, 1)
    light_given = part(chip_terms, 1 - side, block, 1).astype(jnp.bfloat16)

    pre_acts = []
    for name, one in zip(("pre_own", "pre_near", "pre_facing", "pre_near"), sheets):
        pre = dot(one, chip_in)
        if name != "pre_facing":
            pre = lax.optimization_barrier(pre)
        pre_acts.append(pre)
    tall = sheet.shape[0]
    early = jnp.concatenate([pre_acts[1], pre_acts[3], pre_acts[0]], axis=0)
    early = gelu_tanh(early).astype(jnp.bfloat16)
    early = jnp.concatenate([early, lax.ppermute(early, "xh", swap)], axis=1)
    late = gelu_tanh(pre_acts[2]).astype(jnp.bfloat16)
    across = lax.ppermute(late, "xh", swap)
    late = jnp.concatenate([late, across], axis=1)
    near = dot(early[: 2 * tall], group_weight).astype(jnp.bfloat16)
    far = dot(late, group_weight).astype(jnp.bfloat16)
    far, back = lax.optimization_barrier((far, back))
    light_got = lax.ppermute(light_given, "xh", swap)
    light_share = light_kept + light_got.astype(jnp.float32)
    own = lax.optimization_barrier(dot(early[2 * tall :], group_weight))
    from_before = moved(near[:tall], third(1))
    from_after = moved(near[tall:], third(-1))
    from_facing = moved(far, third(2))
    for one in (from_before, from_after, from_facing):
        own = own + one.astype(jnp.float32)
    strip = plane.shape[0]
    leaving = own.astype(jnp.bfloat16)
    total = own[:strip]
    strips = [moved(leaving[k * strip : (k + 1) * strip], second(k)) for k in (1, 2, 3)]
    for one in strips:
        total = total + one.astype(jnp.float32)
    count = 4 * tall
    r = jnp.arange(count, dtype=jnp.int32)
    inner, r_y, r_z = r % strip, r // strip % 4, r // tall
    turn_z, turn_y = (r_z - at_z) % 4, (r_y - at_y) % 4
    place = jnp.where(core == 0, turn_z * 4 + turn_y, turn_y * 4 + turn_z) * strip + inner
    place_other = jnp.where(core == 0, turn_y * 4 + turn_z, turn_z * 4 + turn_y) * strip + inner
    choice = (place[:, None] == r[None, :]).astype(jnp.bfloat16)

    pre_act = jnp.concatenate(pre_acts, axis=0)
    pre_rows = jnp.dot(
        choice.astype(jnp.float32),
        pre_act,
        precision=lax.Precision.HIGHEST,
        preferred_element_type=jnp.float32,
    )

    def both_cores(own, theirs):
        pieces = [own.reshape(-1, 1, strip, units), theirs.reshape(-1, 1, strip, units)]
        return ordered(core == 0, pieces[0], pieces[1], 1).reshape(2 * count, units)

    pre_all = both_cores(pre_rows[:, :units], lax.ppermute(pre_rows[:, units:], "b", swap))
    places = jnp.where(
        core == 0,
        jnp.stack([place, place_other + count]),
        jnp.stack([place_other + count, place]),
    )
    places = places.reshape(2, -1, strip).swapaxes(0, 1).reshape(1, -1)
    grad_out, slope_rows = grad_out_of(pre_all, heavy_out, back, places)
    total, slope_rows, grad_out = lax.optimization_barrier((total, slope_rows, grad_out))
    homed = part(total, low, half, 0) + lax.ppermute(
        part(total, 1 - low, half, 0).astype(jnp.bfloat16), "xl", swap
    ).astype(jnp.float32)
    theirs_sheets = [lax.ppermute(one, "b", swap) for one in sheets]
    grad_in = grad_in_of(list(sheets) + theirs_sheets, slope_rows)
    swapped = lax.ppermute(part(homed, 1 - core, block, 1), "b", swap)
    heavy_share = ordered(core == 0, part(homed, core, block, 1), swapped, 0) * row_scale[:, None]
    naming = (jnp.arange(rows, dtype=jnp.int32)[:, None] == positions[None, :]).astype(jnp.float32)
    spread = jnp.dot(
        naming, heavy_share, precision=lax.Precision.HIGHEST, preferred_element_type=jnp.float32
    )
    mixed = (light_share + spread).astype(jnp.bfloat16)


    return (mixed, grad_in, grad_out)


def solution(mesh):
    split = Mesh(mesh.devices.reshape(*sizes), axes)
    seq = ("z", "y", "xl")
    units = axes
    in_specs = (
        P(seq, "xh"),
        P(None, ("b", "xh")),
        P(("b", "xh"), None),
        P(None, units),
        P(units, None),
        P(seq, None),
        P(seq),
        P(seq, None),
        P(seq, "xh"),
    )
    out_specs = (
        P(seq, ("b", "xh")),
        P(None, units),
        P(units, None),
    )

    return jax.shard_map(
        per_device, mesh=split, in_specs=in_specs, out_specs=out_specs, check_vma=False
    )
```
